32 devices in a mesh: hst: 4 (over y, x), chip: 8 (over z, core).
Axes of the slice: x: 2, y: 2, z: 4, core: 2. Of those that a mesh axis runs over, the one named last changes fastest.
Arguments:
- resident_row_blocks: bfloat16 [1536, 128, 128], P(('hst', 'chip')), may hold values from -3 to 3
- orphan_blocks: bfloat16 [1024, 128, 128], P(('hst', 'chip')), may hold values from -3 to 3
- home_offsets: int32 [1536, 32, 8], P(('hst', 'chip')), may hold values from 0 to 127
- home_lengths: int32 [1536, 32], P(('hst', 'chip')), may hold values from 1 to 8
- home_samples: int32 [1536, 32], P(('hst', 'chip')), may hold values from 0 to 511
- orphan_offsets: int32 [1024, 32, 8], P(('hst', 'chip')), may hold values from 0 to 127
- orphan_lengths: int32 [1024, 32], P(('hst', 'chip')), may hold values from 1 to 8
- orphan_samples: int32 [1024, 32], P(('hst', 'chip')), may hold values from 0 to 511
- orphan_owner: int32 [1024, 1], P(('hst', 'chip')), may hold values from 0 to 7; in each aligned block of 32 rows (0 to 31, 32 to 63, ...) at most 8 rows name the same one
- dense_inputs: bfloat16 [16384, 13], P(('hst', 'chip')), may hold values from -6 to 6
- labels: int32 [16384], P(('hst', 'chip')), may hold values 0 or 1
- bottom_first: bfloat16 [13, 512], replicated, may hold values from -1.75 to 1.75
- bias_first: float32 [512], replicated, may hold values from -1.5 to 1.5
- bottom_second: bfloat16 [512, 256], replicated, may hold values from -0.375 to 0.375
- bias_second: float32 [256], replicated, may hold values from -1.5 to 1.5
- bottom_third: bfloat16 [256, 128], replicated, may hold values from -0.5 to 0.5
- bias_third: float32 [128], replicated, may hold values from -1.5 to 1.5
- top_hidden: bfloat16 [479, 1024], replicated, may hold values from -0.125 to 0.125
- bias_hidden: float32 [1024], replicated, may hold values from -1.5 to 1.5
- top_logit: bfloat16 [1024, 1], replicated, may hold values from -0.25 to 0.25
- bias_logit: float32 [1], replicated, may hold values from -3 to 3
Outputs:
- rehomed: bfloat16 [2048, 128, 128], P(('hst', 'chip'))
- logits: float32 [16384], P(('hst', 'chip'))
- loss: float32 [], replicated
The draws below stay inside these ranges and needn't reach their ends.
Inputs may be any that keep to these rules, and one draw needn't show every extreme that they name: `orphan_owner`: among the 32 orphans of one device at most 8 have the same new owner; some holder and owner reach 8.
All inputs are finite; a program needn't handle non-finite values. No bound on the sum of `labels` on one device may be relied on, other than what follows from the above.
Results may differ from the reference program's by a relative error of at most 0.0079.
Values may be sent and summed in bfloat16 or wider, within the bound.
A program may use at most 128 MiB of HBM per device.

```python
import math
import jax
import jax.numpy as jnp
import numpy as np
from jax import lax

E = 128
F = 26
DENSE = 13
BOT1 = 512
BOT2 = 256
TOP1 = 1024
BR = 128
L = 8
ORPH_DEV = 32
BATCH_DEV = 512
SLOT = 8
RECV = 64
PIECES = 32
RESIDENT = 1536
ORPHANS = 1024
BATCH = 16384
INTER = 479
N_HST = 4
N_CHIP = 8
DEVICES = 32


def touch_ends(result, stream_key, low, high):
    shape = result.shape
    index_at = [jax.random.randint(jax.random.fold_in(stream_key, axis), (), 0, shape[axis]) for axis in range(len(shape))]
    result = result.at[tuple(index_at)].set(low)
    longest = shape.index(max(shape))
    index_at[longest] = (index_at[longest] + 1) % shape[longest]
    return result.at[tuple(index_at)].set(high)


def levels(rng, dims, cuts, low, top_value):
    loudness = 1.0
    for position, blocks in cuts:
        steps = jax.random.uniform(jax.random.fold_in(jax.random.fold_in(rng, 6), position), (blocks,), jnp.float32, low / len(cuts), top_value / len(cuts))
        loudness = loudness * jnp.repeat(jnp.exp(steps), dims[position] // blocks).reshape((-1,) + (1,) * (len(dims) - 1 - position))
    return loudness


def shared_out(own_key, own, number, rows, number_of, top, bound, slope):
    ranking = jax.random.permutation(own_key, number_of)
    heavy_load, ordinary = portions_of(number_of, rows * top, bound, slope, True), portions_of(number_of, rows * top, bound, slope, False)
    places = jnp.arange(number_of)

    def named(tallies, turn):
        used = int((tallies > 0).sum())
        fixed = max(1, used // 4)
        shifted = fixed + (places - fixed + turn * (used - fixed)) % max(1, number_of - fixed)
        return jnp.zeros((number_of,), jnp.int32).at[ranking[jnp.where(places < fixed, places, shifted)]].set(jnp.asarray(tallies, jnp.int32))

    tallies = jnp.where(number % 4 == 0, named(heavy_load, number // 4), named(ordinary, number - number // 4 - 1))
    mixed = jax.random.permutation(jax.random.fold_in(own, 3), number_of)
    donor, taker = mixed[0:number_of // 2 * 2:2], mixed[1:number_of // 2 * 2:2]
    slack = jnp.minimum(tallies[donor] - 1, bound - tallies[taker]) // 2
    slack = jnp.where((donor == ranking[0]) | (taker == ranking[0]) | (tallies[taker] == 0), 0, jnp.maximum(slack, 0))
    shifted = jax.random.randint(jax.random.fold_in(own, 4), (number_of // 2,), 0, 1 << 20) % (slack + 1)
    tallies = tallies.at[donor].add(-shifted).at[taker].add(shifted)
    items = jnp.searchsorted(jnp.cumsum(tallies), jnp.arange(rows * top), side="right").astype(jnp.int32)
    listing = items.reshape(top, rows).T
    listing = listing[jax.random.permutation(jax.random.fold_in(own, 1), rows)]
    turn = jax.random.randint(jax.random.fold_in(own, 2), (rows, 1), 0, top)
    return jnp.take_along_axis(listing, (jnp.arange(top)[None, :] + turn) % top, axis=1)


def portions_of(count, total, limit, slope, full):
    portions = [(1 << 20) // math.isqrt(standing ** slope) + 1 for standing in range(1, count + 1)]
    largest = limit if full else min(limit, max(-(-total // count), total * portions[0] // sum(portions)))
    least = 1 if total - largest >= count - 1 else 0
    given, surplus = [largest] + [least] * (count - 1), total - largest - least * (count - 1)
    while surplus > 0:
        candidates = [i for i in range(1, count) if given[i] < largest] or [i for i in range(1, count) if given[i] < limit]
        mass, remaining = sum([portions[i] for i in candidates]), surplus
        for i in candidates:
            addition = min(limit - given[i], max(1, remaining * portions[i] // mass), surplus)
            given[i] = given[i] + addition
            surplus = surplus - addition
    return np.array(given)


def gaussian(key, dims, scale, reach, split=(), held_as=jnp.bfloat16):
    values = jax.random.normal(key, dims, jnp.float32) * scale
    if len(split) > 0:
        values = levels(key, dims, split, -0.22, 0.18) * values
    return jnp.clip(values, min=-reach, max=reach).astype(held_as)


def setup_inputs(seed: int = 0) -> dict:
    seeds = jax.random.split(jax.random.key(seed), 22)
    resident_row_blocks = gaussian(seeds[0], (RESIDENT, BR, E), 0.5, 3.0, ((0, 32),))
    orphan_blocks = gaussian(seeds[1], (ORPHANS, BR, E), 0.5, 3.0, ((0, 32),))
    home_offsets = touch_ends(jax.random.randint(seeds[2], (RESIDENT, PIECES, L), 0, BR), jax.random.fold_in(seeds[2], 1), 0, BR - 1).astype(jnp.int32)
    home_lengths = touch_ends(jax.random.randint(seeds[3], (RESIDENT, PIECES), 1, L + 1), jax.random.fold_in(seeds[3], 1), 1, L).astype(jnp.int32)
    home_samples = touch_ends(jax.random.randint(seeds[4], (RESIDENT, PIECES), 0, BATCH_DEV), jax.random.fold_in(seeds[4], 1), 0, BATCH_DEV - 1).astype(jnp.int32)
    orphan_offsets = touch_ends(jax.random.randint(seeds[5], (ORPHANS, PIECES, L), 0, BR), jax.random.fold_in(seeds[5], 1), 0, BR - 1).astype(jnp.int32)
    orphan_lengths = touch_ends(jax.random.randint(seeds[6], (ORPHANS, PIECES), 1, L + 1), jax.random.fold_in(seeds[6], 1), 1, L).astype(jnp.int32)
    orphan_samples = touch_ends(jax.random.randint(seeds[7], (ORPHANS, PIECES), 0, BATCH_DEV), jax.random.fold_in(seeds[7], 1), 0, BATCH_DEV - 1).astype(jnp.int32)
    orphan_owner_keys = jax.random.split(jax.random.fold_in(seeds[8], 1), ORPHANS // ORPH_DEV)
    orphan_owner_turns = jax.random.permutation(jax.random.fold_in(seeds[8], 3), ORPHANS // ORPH_DEV)
    orphan_owner = jax.vmap(lambda own, number: shared_out(jax.random.fold_in(seeds[8], 2), own, number, ORPH_DEV, N_CHIP, 1, SLOT, 2))(orphan_owner_keys, orphan_owner_turns).reshape((ORPHANS, 1))
    dense_inputs = gaussian(seeds[9], (BATCH, DENSE), 1.0, 6.0, ((0, 32),))
    labels = touch_ends((jax.random.randint(seeds[10], (BATCH,), 0, 2) < 1).astype(jnp.int32), jax.random.fold_in(seeds[10], 1), 0, 1)
    bottom_first = gaussian(seeds[11], (DENSE, BOT1), DENSE ** -0.5, 1.75)
    bias_first = gaussian(seeds[12], (BOT1,), 0.3, 1.5, (), jnp.float32)
    bottom_second = gaussian(seeds[13], (BOT1, BOT2), (BOT1 // 2) ** -0.5, 0.375)
    bias_second = gaussian(seeds[14], (BOT2,), 0.3, 1.5, (), jnp.float32)
    bottom_third = gaussian(seeds[15], (BOT2, E), (BOT2 // 2) ** -0.5, 0.5)
    bias_third = gaussian(seeds[16], (E,), 0.3, 1.5, (), jnp.float32)
    top_hidden = gaussian(seeds[17], (INTER, TOP1), (INTER * 4) ** -0.5, 0.125)
    bias_hidden = gaussian(seeds[18], (TOP1,), 0.3, 1.5, (), jnp.float32)
    top_logit = gaussian(seeds[19], (TOP1, 1), (TOP1 // 2) ** -0.5, 0.25)
    bias_logit = gaussian(seeds[20], (1,), 1.0, 3.0, (), jnp.float32)
    return dict(resident_row_blocks=resident_row_blocks, orphan_blocks=orphan_blocks, home_offsets=home_offsets, home_lengths=home_lengths, home_samples=home_samples, orphan_offsets=orphan_offsets, orphan_lengths=orphan_lengths, orphan_samples=orphan_samples, orphan_owner=orphan_owner, dense_inputs=dense_inputs, labels=labels, bottom_first=bottom_first, bias_first=bias_first, bottom_second=bottom_second, bias_second=bias_second, bottom_third=bottom_third, bias_third=bias_third, top_hidden=top_hidden, bias_hidden=bias_hidden, top_logit=top_logit, bias_logit=bias_logit)


def pool_one(block, offsets, lengths):
    rows = jnp.arange(block.shape[0], dtype=jnp.int32)
    places = jnp.arange(offsets.shape[1], dtype=jnp.int32)
    hit = (offsets[:, :, None] == rows[None, None, :]) & (places[None, :, None] < lengths[:, None, None])
    counts = jnp.sum(hit.astype(jnp.float32), axis=1)
    return jnp.dot(counts.astype(jnp.bfloat16), block, preferred_element_type=jnp.float32).astype(jnp.bfloat16)


def slot_provenance(owners):
    count = owners.shape[0]
    index = jnp.arange(count, dtype=jnp.int32)
    earlier = index[None, :] < index[:, None]
    rank = jnp.sum(((owners[:, None] == owners[None, :]) & earlier).astype(jnp.int32), axis=1).astype(jnp.int32)
    flat = owners * SLOT + rank
    match = flat[None, :] == jnp.arange(RECV, dtype=jnp.int32)[:, None]
    source = jnp.sum(match.astype(jnp.int32) * index[None, :], axis=1).astype(jnp.int32)
    return source, jnp.any(match, axis=1)


def reference(resident_row_blocks, orphan_blocks, home_offsets, home_lengths, home_samples, orphan_offsets, orphan_lengths, orphan_samples, orphan_owner, dense_inputs, labels, bottom_first, bias_first, bottom_second, bias_second, bottom_third, bias_third, top_hidden, bias_hidden, top_logit, bias_logit):
    grouped = orphan_blocks.reshape(DEVICES, ORPH_DEV, BR, E)
    owners = orphan_owner[:, 0].reshape(DEVICES, ORPH_DEV)

    def outgoing(blocks, targets):
        source, filled = slot_provenance(targets)
        return jnp.where(filled[:, None, None], blocks[source], jnp.zeros((), jnp.bfloat16))

    buffers = jax.vmap(outgoing)(grouped, owners)
    buffers = buffers.reshape(N_HST, N_CHIP, N_CHIP, SLOT, BR, E).transpose(0, 2, 1, 3, 4, 5)
    rehomed = buffers.reshape(DEVICES * RECV, BR, E)

    blocks = jnp.concatenate([resident_row_blocks, orphan_blocks], axis=0)
    offsets = jnp.concatenate([home_offsets, orphan_offsets], axis=0)
    lengths = jnp.concatenate([home_lengths, orphan_lengths], axis=0)
    samples = jnp.concatenate([home_samples, orphan_samples], axis=0)
    ids = jnp.arange(blocks.shape[0], dtype=jnp.int32)
    feature = ids % F
    piece = lax.map(lambda item: pool_one(item[0], item[1], item[2]), (blocks, offsets, lengths))
    owner = jnp.arange(PIECES, dtype=jnp.int32)
    target = (owner[None, :] * BATCH_DEV + samples) * F + feature[:, None]
    pooled = jax.ops.segment_sum(piece.reshape(-1, E).astype(jnp.float32), target.reshape(-1).astype(jnp.int32), num_segments=BATCH * F)
    pooled = pooled.reshape(BATCH, F, E)

    first = jax.nn.relu(jnp.dot(dense_inputs, bottom_first, preferred_element_type=jnp.float32) + bias_first).astype(jnp.bfloat16)
    second = jax.nn.relu(jnp.dot(first, bottom_second, preferred_element_type=jnp.float32) + bias_second).astype(jnp.bfloat16)
    bottom = jax.nn.relu(jnp.dot(second, bottom_third, preferred_element_type=jnp.float32) + bias_third)
    stacked_vectors = jnp.concatenate([bottom[:, None, :], pooled], axis=1).astype(jnp.bfloat16)
    widened_features = stacked_vectors.astype(jnp.float32)
    pairwise_products = jnp.einsum("asu,adu->asd", widened_features, widened_features)
    lower_i, lower_j = np.tril_indices(F + 1, -1)
    pairs = pairwise_products[:, lower_i, lower_j]
    feature_vectors = jnp.concatenate([bottom, pairs], axis=1).astype(jnp.bfloat16)
    hidden = jax.nn.relu(jnp.dot(feature_vectors, top_hidden, preferred_element_type=jnp.float32) + bias_hidden).astype(jnp.bfloat16)
    logits = jnp.dot(hidden, top_logit, preferred_element_type=jnp.float32)[:, 0] + bias_logit[0]
    loss = jnp.sum(jax.nn.softplus(logits) - labels.astype(jnp.float32) * logits)
    return rehomed, logits, loss
```

```python
import functools

import jax
import jax.numpy as jnp
from jax import lax
from jax.experimental import pallas as pl
from jax.experimental.pallas import tpu as pltpu
from jax.sharding import PartitionSpec as P

F = 26
SLAB = 32
VM = pltpu.VMEM
F32, BF16, I32 = jnp.float32, jnp.bfloat16, jnp.int32


def cost(flops, bytes_accessed):
    return pl.CostEstimate(flops=flops, bytes_accessed=bytes_accessed, transcendentals=0)


def nt(a, b):
    return lax.dot_general(a, b, (((1,), (1,)), ((), ())), preferred_element_type=F32)


def mm(a, b):
    return jnp.dot(a, b, preferred_element_type=F32)


def place_kernel(slots, owner_ref, blocks_ref, out_ref, used):
    chips = out_ref.shape[0] // slots
    out_ref[...] = jnp.zeros_like(out_ref)
    for c in range(chips):
        used[c] = 0

    def step(i, carry):
        c = owner_ref[i]
        rank = used[c]
        used[c] = rank + 1
        out_ref[c * slots + rank] = blocks_ref[i]
        return carry

    lax.fori_loop(0, blocks_ref.shape[0], step, 0)


def place(owners, blocks, chips, slots):
    shape = (chips * slots,) + blocks.shape[1:]
    return pl.pallas_call(
        functools.partial(place_kernel, slots),
        out_shape=jax.ShapeDtypeStruct(shape, blocks.dtype),
        in_specs=[pl.BlockSpec(memory_space=pltpu.SMEM), pl.BlockSpec(memory_space=VM)],
        out_specs=pl.BlockSpec(memory_space=VM),
        scratch_shapes=[pltpu.SMEM((chips,), I32)],
        cost_estimate=cost(1000, 3 * blocks.size * 2),
        name="place",
    )(owners, blocks)


def pool_kernel(peers, stride, off_ref, samp_ref, home_ref, orph_ref, out_ref, rows_ref):
    homes, height = home_ref.shape[0], home_ref.shape[1]
    count = homes + orph_ref.shape[0]
    per = 128 // peers
    row = lax.broadcasted_iota(I32, (height, 128), 0)
    rows_ref[...] = jnp.zeros_like(rows_ref)
    samp = samp_ref[...]
    rows_ref[pl.ds(count, peers, stride=stride), :] = (samp // 256).astype(F32)
    rows_ref[pl.ds(count + 1, peers, stride=stride), :] = (samp % 256).astype(F32)

    def group(block_ref, base):
        def step(g, carry):
            first = base + g * per
            lanes = pl.ds(pl.multiple_of(first * peers, 128), 128)
            hits = jnp.zeros((height, 128), F32)
            for place_ in range(off_ref.shape[0]):
                hits = hits + (row == off_ref[place_:place_ + 1, lanes]).astype(F32)
            counts = hits.T.astype(BF16)
            for k in range(per):
                piece = mm(counts[k * peers:(k + 1) * peers], block_ref[g * per + k])
                rows_ref[pl.ds(first + k, peers, stride=stride), :] = piece
            return carry

        lax.fori_loop(0, block_ref.shape[0] // per, step, 0, unroll=2)

    group(home_ref, 0)
    group(orph_ref, homes)
    out_ref[...] = rows_ref[...].astype(BF16)


def pool(off, samp, home, orph, peers, stride):
    width = home.shape[2]
    return pl.pallas_call(
        functools.partial(pool_kernel, peers, stride),
        out_shape=jax.ShapeDtypeStruct((peers * stride, width), BF16),
        in_specs=[pl.BlockSpec(memory_space=VM)] * 4,
        out_specs=pl.BlockSpec(memory_space=VM),
        scratch_shapes=[VM((peers * stride, width), F32)],
        cost_estimate=cost(2 * peers * (home.size + orph.size), 4 * home.size),
        name="pool",
    )(off, samp, home, orph)


def top_kernel(
    homes, orphs, depth,
    arr_ref, samp_ref, dense_ref, w1_ref, b1_ref, w2_ref, b2_ref, w3_ref, b3_ref,
    wt_ref, bh_ref, wl_ref, bl_ref, label_ref,
    logit_ref, loss_ref,
    pieces, slab, gram, wpad, wexp,
):
    peers = arr_ref.shape[0]
    batch = dense_ref.shape[0]
    inter = wt_ref.shape[0]
    total = peers * (homes + orphs)

    whole = inter // 16 * 16
    wpad[whole:, :] = jnp.zeros((wpad.shape[0] - whole, wpad.shape[1]), BF16)
    wpad[0:inter, :] = wt_ref[...]
    slot = lax.broadcasted_iota(I32, (SLAB * SLAB, wpad.shape[0]), 0)
    i, j = slot // SLAB, slot % SLAB
    column = lax.broadcasted_iota(I32, slot.shape, 1)
    pick = (column == 128 + i * (i - 1) // 2 + j) & (j < i) & (i <= F)
    wexp[...] = mm(jnp.where(pick, 1.0, 0.0).astype(BF16), wpad[...]).astype(BF16)

    first = jnp.maximum(mm(dense_ref[...], w1_ref[...]) + b1_ref[...], 0.0).astype(BF16)
    second = jnp.maximum(mm(first, w2_ref[...]) + b2_ref[...], 0.0).astype(BF16)
    bottom = jnp.maximum(mm(second, w3_ref[...]) + b3_ref[...], 0.0)
    slab[0] = bottom
    slab[F + 1:] = jnp.zeros((SLAB - F - 1,) + slab.shape[1:], F32)

    pieces[total:, :] = jnp.zeros((pieces.shape[0] - total, pieces.shape[1]), F32)

    def settle(p, carry):
        pieces[pl.ds(pl.multiple_of(p * homes, 8), homes), :] = arr_ref[p, 0:homes].astype(F32)
        pieces[pl.ds(pl.multiple_of(peers * homes + p * orphs, 8), orphs), :] = (
            arr_ref[p, homes:homes + orphs].astype(F32))
        return carry

    lax.fori_loop(0, peers, settle, 0, unroll=2)

    sample = lax.broadcasted_iota(I32, (batch, depth), 0)
    for f in range(F):
        mine = pieces[pl.ds(f, depth, stride=F), :].astype(BF16)
        hot = jnp.where(sample == samp_ref[f:f + 1, :], 1.0, 0.0).astype(BF16)
        slab[f + 1] = mm(hot, mine)

    edge = SLAB * 8
    same = (lax.broadcasted_iota(I32, (edge, edge), 0) % 8) == (
        lax.broadcasted_iota(I32, (edge, edge), 1) % 8)

    def products(g, carry):
        halves = []
        for k in range(2):
            at = pl.ds(pl.multiple_of(g * 16 + k * 8, 8), 8)
            x = slab[:, at, :].reshape(edge, slab.shape[2]).astype(BF16)
            halves.append(jnp.where(same, nt(x, x), 0.0).reshape(SLAB, 8, edge))
        both = jnp.concatenate(halves, axis=1).astype(BF16)
        gram[:, pl.ds(pl.multiple_of(g * 16, 16), 16), :] = both
        return carry

    lax.fori_loop(0, batch // 16, products, 0, unroll=2)

    lane_j = lax.broadcasted_iota(I32, (edge, edge), 0) // 8
    out_lane = lax.broadcasted_iota(I32, (edge, edge), 1)
    features = []
    for h in range(SLAB // 8):
        acc = None
        for k in range(8):
            i_ = h * 8 + k
            if i_ < 1 or i_ > F:
                continue
            live = 128 if i_ <= 16 else edge
            fold = jnp.where(lane_j + k * SLAB == out_lane, 1.0, 0.0).astype(BF16)
            term = mm(gram[i_, :, 0:live], fold[0:live])
            acc = term if acc is None else acc + term
        features.append(acc.astype(BF16))
    bottom = slab[0].astype(BF16)

    part = jnp.zeros((batch, 128), F32)
    step = 256
    for n in range(0, wt_ref.shape[1], step):
        pre = mm(bottom, wpad[0:128, n:n + step])
        for h in range(SLAB // 8):
            pre = pre + mm(features[h], wexp[h * 256:(h + 1) * 256, n:n + step])
        hidden = jnp.maximum(pre + bh_ref[:, n:n + step], 0.0).astype(BF16).astype(F32)
        scaled = hidden * wl_ref[:, n:n + step]
        part = part + scaled[:, 0:128] + scaled[:, 128:256]
    logits = jnp.sum(part.T, axis=0, keepdims=True) + bl_ref[0]
    logit_ref[...] = logits
    soft = jnp.maximum(logits, 0.0) + jnp.log1p(jnp.exp(-jnp.abs(logits)))
    loss = jnp.sum(soft - label_ref[...].astype(F32) * logits, axis=1, keepdims=True)
    loss_ref[...] = jnp.broadcast_to(loss, loss_ref.shape)


def top(homes, orphs, depth, arrived, samp, dense, w1, b1, w2, b2, w3, b3, wt, bh, wl, bl, labels):
    peers, _, width = arrived.shape
    batch = dense.shape[0]
    vmem = pl.BlockSpec(memory_space=VM)
    return pl.pallas_call(
        functools.partial(top_kernel, homes, orphs, depth),
        out_shape=(
            jax.ShapeDtypeStruct((1, batch), F32),
            jax.ShapeDtypeStruct((peers, 128), F32),
        ),
        in_specs=[vmem] * 12 + [pl.BlockSpec(memory_space=pltpu.SMEM), vmem],
        out_specs=(vmem, vmem),
        scratch_shapes=[
            VM((F * depth, width), F32),
            VM((SLAB, batch, width), F32),
            VM((SLAB, batch, SLAB * 8), BF16),
            VM((512, wt.shape[1]), BF16),
            VM((SLAB * SLAB, wt.shape[1]), BF16),
        ],
        cost_estimate=cost(8_000_000_000, 8_000_000),
        name="top",
    )(arrived, samp, dense, w1, b1, w2, b2, w3, b3, wt, bh, wl, bl, labels)


def per_device(
    resident_row_blocks,
    orphan_blocks,
    home_offsets,
    home_lengths,
    home_samples,
    orphan_offsets,
    orphan_lengths,
    orphan_samples,
    orphan_owner,
    dense_inputs,
    labels,
    bottom_first,
    bias_first,
    bottom_second,
    bias_second,
    bottom_third,
    bias_third,
    top_hidden,
    bias_hidden,
    top_logit,
    bias_logit,
):
    chips = lax.axis_size("chip")
    devices = lax.axis_size("hst") * chips
    everyone = ("hst", "chip")
    homes, orphs = resident_row_blocks.shape[0], orphan_blocks.shape[0]
    height, width = resident_row_blocks.shape[1:]
    batch = dense_inputs.shape[0]
    slots = (2 * orphs + chips - 1) // chips
    count = homes + orphs
    stride = -(-(count + 2) // 16) * 16

    outgoing = place(orphan_owner[:, 0], orphan_blocks, chips, slots)
    rehomed = lax.all_to_all(outgoing, "chip", split_axis=0, concat_axis=0, tiled=True)

    offsets = jnp.concatenate([home_offsets, orphan_offsets], axis=0)
    lengths = jnp.concatenate([home_lengths, orphan_lengths], axis=0)
    samples = jnp.concatenate([home_samples, orphan_samples], axis=0)
    live = jnp.arange(offsets.shape[2], dtype=I32) < lengths[:, :, None]
    off = jnp.where(live, offsets, height).transpose(2, 0, 1).reshape(offsets.shape[2], -1)
    samp = jnp.pad(samples.T, ((0, 0), (0, 128 - count)))

    packed = pool(off, samp, resident_row_blocks, orphan_blocks, devices, stride)
    packed = packed.reshape(devices, stride, width)
    arrived = lax.all_to_all(packed, everyone, split_axis=0, concat_axis=0, tiled=True)

    total = devices * count
    depth = -(-total // (F * 128)) * 128
    where = (arrived[:, count, :count].astype(F32) * 256.0
             + arrived[:, count + 1, :count].astype(F32)).astype(I32)
    where = jnp.concatenate([where[:, :homes].reshape(-1), where[:, homes:].reshape(-1)])
    where = jnp.pad(where, (0, F * depth - total), constant_values=-1).reshape(depth, F).T

    logits, loss = top(
        homes, orphs, depth, arrived, where, dense_inputs,
        bottom_first, bias_first[None], bottom_second, bias_second[None],
        bottom_third, bias_third[None], top_hidden, bias_hidden[None],
        top_logit.T.astype(F32), bias_logit, labels[None],
    )
    losses = lax.all_to_all(loss[:, None, :], everyone, split_axis=0, concat_axis=0, tiled=True)
    return rehomed, logits[0], jnp.sum(losses[:, 0, 0])


def solution(mesh):
    both = ("hst", "chip")
    three, two = P(both, None, None), P(both, None)
    return jax.shard_map(
        per_device,
        mesh=mesh,
        in_specs=(three, three, three, two, two, three, two, two, two, two, P(both)) + (P(),) * 10,
        out_specs=(three, P(both), P()),
        check_vma=False,
    )
```

```python
import functools

import jax
import jax.numpy as jnp
from jax import lax
from jax.experimental import pallas as pl
from jax.experimental.pallas import tpu as pltpu
from jax.sharding import PartitionSpec as P


F = 26
SLAB = 32
VM = pltpu.VMEM
F32, BF16, I32 = jnp.float32, jnp.bfloat16, jnp.int32


def cost(flops, bytes_accessed):
    return pl.CostEstimate(flops=flops, bytes_accessed=bytes_accessed, transcendentals=0)


def nt(a, b):
    return lax.dot_general(a, b, (((1,), (1,)), ((), ())), preferred_element_type=F32)


def mm(a, b):
    return jnp.dot(a, b, preferred_element_type=F32)


def place_kernel(me_ref, owner_ref, blocks_ref, *rest):
    outs, buf, used = rest[:-2], rest[-2], rest[-1]
    chips, slots = len(outs), outs[0].shape[0]
    buf[...] = jnp.zeros_like(buf)
    for c in range(chips):
        used[c] = 0

    def step(i, carry):
        c = lax.rem(owner_ref[i] - me_ref[0] + chips, chips)
        rank = used[c]
        used[c] = rank + 1
        buf[c * slots + rank] = blocks_ref[i]
        return carry

    lax.fori_loop(0, blocks_ref.shape[0], step, 0)
    for k, out in enumerate(outs):
        out[...] = buf[k * slots:(k + 1) * slots]


def place(me, owners, blocks, chips, slots):
    shape = (slots,) + blocks.shape[1:]
    smem, vmem = pl.BlockSpec(memory_space=pltpu.SMEM), pl.BlockSpec(memory_space=VM)
    return pl.pallas_call(
        place_kernel,
        out_shape=[jax.ShapeDtypeStruct(shape, blocks.dtype)] * chips,
        in_specs=[smem, smem, vmem],
        out_specs=[vmem] * chips,
        scratch_shapes=[VM((chips * slots,) + blocks.shape[1:], blocks.dtype), pltpu.SMEM((chips,), I32)],
        cost_estimate=cost(1000, 3 * blocks.size * 2),
        compiler_params=pltpu.CompilerParams(vmem_limit_bytes=12 * 2**20),
        name="place",
    )(me, owners, blocks)


def gather_kernel(me_ref, *rest):
    ins, out_ref, sems = rest[:-2], rest[-2], rest[-1]
    chips, slots = len(ins), ins[0].shape[0]
    copies = []
    for k, ref in enumerate(ins):
        holder = lax.rem(me_ref[0] - k + chips, chips)
        copies.append(pltpu.make_async_copy(ref, out_ref.at[pl.ds(holder * slots, slots)], sems.at[k]))
    for copy in copies:
        copy.start()
    for copy in copies:
        copy.wait()


def gather(me, parts):
    shape = (len(parts) * parts[0].shape[0],) + parts[0].shape[1:]
    vmem = pl.BlockSpec(memory_space=VM)
    return pl.pallas_call(
        gather_kernel,
        out_shape=jax.ShapeDtypeStruct(shape, parts[0].dtype),
        in_specs=[pl.BlockSpec(memory_space=pltpu.SMEM)] + [vmem] * len(parts),
        out_specs=pl.BlockSpec(memory_space=pl.ANY),
        scratch_shapes=[pltpu.SemaphoreType.DMA((len(parts),))],
        cost_estimate=cost(1000, 4 * len(parts) * parts[0].size),
        compiler_params=pltpu.CompilerParams(vmem_limit_bytes=8 * 2**20),
        name="gather",
    )(me, *parts)


def pool_kernel(peers, stride, off_ref, samp_ref, home_ref, orph_ref, out_ref, rows_ref):
    homes, height = home_ref.shape[0], home_ref.shape[1]
    count = homes + orph_ref.shape[0]
    per = 128 // peers
    row = lax.broadcasted_iota(I32, (height, 128), 0)
    rows_ref[...] = jnp.zeros_like(rows_ref)
    samp = samp_ref[...]
    rows_ref[pl.ds(count, peers, stride=stride), :] = (samp // 256).astype(F32)
    rows_ref[pl.ds(count + 1, peers, stride=stride), :] = (samp % 256).astype(F32)

    def group(block_ref, base):
        def step(g, carry):
            first = base + g * per
            lanes = pl.ds(pl.multiple_of(first * peers, 128), 128)
            hits = jnp.zeros((height, 128), F32)
            for place_ in range(off_ref.shape[0]):
                hits = hits + (row == off_ref[place_:place_ + 1, lanes]).astype(F32)
            counts = hits.T.astype(BF16)
            for k in range(per):
                piece = mm(counts[k * peers:(k + 1) * peers], block_ref[g * per + k])
                rows_ref[pl.ds(first + k, peers, stride=stride), :] = piece
            return carry

        lax.fori_loop(0, block_ref.shape[0] // per, step, 0, unroll=2)

    group(home_ref, 0)
    group(orph_ref, homes)
    out_ref[...] = rows_ref[...].astype(BF16)


def pool(off, samp, home, orph, peers, stride):
    width = home.shape[2]
    return pl.pallas_call(
        functools.partial(pool_kernel, peers, stride),
        out_shape=jax.ShapeDtypeStruct((peers * stride, width), BF16),
        in_specs=[pl.BlockSpec(memory_space=VM)] * 4,
        out_specs=pl.BlockSpec(memory_space=VM),
        scratch_shapes=[VM((peers * stride, width), F32)],
        cost_estimate=cost(2 * peers * (home.size + orph.size), 4 * home.size),
        compiler_params=pltpu.CompilerParams(vmem_limit_bytes=20 * 2**20),
        name="pool",
    )(off, samp, home, orph)


def top_kernel(
    homes, orphs, depth,
    arr_ref, samp_ref, dense_ref, w1_ref, b1_ref, w2_ref, b2_ref, w3_ref, b3_ref,
    wt_ref, bh_ref, wl_ref, bl_ref, label_ref,
    logit_ref, loss_ref,
    pieces, slab, gram, wpad, wexp,
):
    peers = arr_ref.shape[0]
    batch = dense_ref.shape[0]
    inter = wt_ref.shape[0]
    total = peers * (homes + orphs)

    whole = inter // 16 * 16
    wpad[whole:, :] = jnp.zeros((wpad.shape[0] - whole, wpad.shape[1]), BF16)
    wpad[0:inter, :] = wt_ref[...]
    slot = lax.broadcasted_iota(I32, (SLAB * SLAB, wpad.shape[0]), 0)
    i, j = slot // SLAB, slot % SLAB
    column = lax.broadcasted_iota(I32, slot.shape, 1)
    pick = (column == 128 + i * (i - 1) // 2 + j) & (j < i) & (i <= F)
    wexp[...] = mm(jnp.where(pick, 1.0, 0.0).astype(BF16), wpad[...]).astype(BF16)

    first = jnp.maximum(mm(dense_ref[...], w1_ref[...]) + b1_ref[...], 0.0).astype(BF16)
    second = jnp.maximum(mm(first, w2_ref[...]) + b2_ref[...], 0.0).astype(BF16)
    bottom = jnp.maximum(mm(second, w3_ref[...]) + b3_ref[...], 0.0)
    slab[0] = bottom
    slab[F + 1:] = jnp.zeros((SLAB - F - 1,) + slab.shape[1:], F32)

    pieces[total:, :] = jnp.zeros((pieces.shape[0] - total, pieces.shape[1]), F32)

    def settle(p, carry):
        pieces[pl.ds(pl.multiple_of(p * homes, 8), homes), :] = arr_ref[p, 0:homes].astype(F32)
        pieces[pl.ds(pl.multiple_of(peers * homes + p * orphs, 8), orphs), :] = (
            arr_ref[p, homes:homes + orphs].astype(F32))
        return carry

    lax.fori_loop(0, peers, settle, 0, unroll=2)

    sample = lax.broadcasted_iota(I32, (batch, depth), 0)
    for f in range(F):
        mine = pieces[pl.ds(f, depth, stride=F), :].astype(BF16)
        hot = jnp.where(sample == samp_ref[f:f + 1, :], 1.0, 0.0).astype(BF16)
        slab[f + 1] = mm(hot, mine)

    edge = SLAB * 8
    same = (lax.broadcasted_iota(I32, (edge, edge), 0) % 8) == (
        lax.broadcasted_iota(I32, (edge, edge), 1) % 8)

    def products(g, carry):
        halves = []
        for k in range(2):
            at = pl.ds(pl.multiple_of(g * 16 + k * 8, 8), 8)
            x = slab[:, at, :].reshape(edge, slab.shape[2]).astype(BF16)
            halves.append(jnp.where(same, nt(x, x), 0.0).reshape(SLAB, 8, edge))
        both = jnp.concatenate(halves, axis=1).astype(BF16)
        gram[:, pl.ds(pl.multiple_of(g * 16, 16), 16), :] = both
        return carry

    lax.fori_loop(0, batch // 16, products, 0, unroll=2)

    lane_j = lax.broadcasted_iota(I32, (edge, edge), 0) // 8
    out_lane = lax.broadcasted_iota(I32, (edge, edge), 1)
    features = []
    for h in range(SLAB // 8):
        acc = None
        for k in range(8):
            i_ = h * 8 + k
            if i_ < 1 or i_ > F:
                continue
            live = 128 if i_ <= 16 else edge
            fold = jnp.where(lane_j + k * SLAB == out_lane, 1.0, 0.0).astype(BF16)
            term = mm(gram[i_, :, 0:live], fold[0:live])
            acc = term if acc is None else acc + term
        features.append(acc.astype(BF16))
    bottom = slab[0].astype(BF16)

    part = jnp.zeros((batch, 128), F32)
    step = 256
    for n in range(0, wt_ref.shape[1], step):
        pre = mm(bottom, wpad[0:128, n:n + step])
        for h in range(SLAB // 8):
            pre = pre + mm(features[h], wexp[h * 256:(h + 1) * 256, n:n + step])
        hidden = jnp.maximum(pre + bh_ref[:, n:n + step], 0.0).astype(BF16).astype(F32)
        scaled = hidden * wl_ref[:, n:n + step]
        part = part + scaled[:, 0:128] + scaled[:, 128:256]
    logits = jnp.sum(part.T, axis=0, keepdims=True) + bl_ref[0]
    logit_ref[...] = logits
    soft = jnp.maximum(logits, 0.0) + jnp.log1p(jnp.exp(-jnp.abs(logits)))
    loss = jnp.sum(soft - label_ref[...].astype(F32) * logits, axis=1, keepdims=True)
    loss_ref[...] = jnp.broadcast_to(loss, loss_ref.shape)


def top(homes, orphs, depth, arrived, samp, dense, w1, b1, w2, b2, w3, b3, wt, bh, wl, bl, labels):
    peers, _, width = arrived.shape
    batch = dense.shape[0]
    vmem = pl.BlockSpec(memory_space=VM)
    return pl.pallas_call(
        functools.partial(top_kernel, homes, orphs, depth),
        out_shape=(
            jax.ShapeDtypeStruct((1, batch), F32),
            jax.ShapeDtypeStruct((peers, 128), F32),
        ),
        in_specs=[vmem] * 12 + [pl.BlockSpec(memory_space=pltpu.SMEM), vmem],
        out_specs=(vmem, vmem),
        scratch_shapes=[
            VM((F * depth, width), F32),
            VM((SLAB, batch, width), F32),
            VM((SLAB, batch, SLAB * 8), BF16),
            VM((512, wt.shape[1]), BF16),
            VM((SLAB * SLAB, wt.shape[1]), BF16),
        ],
        cost_estimate=cost(8_000_000_000, 8_000_000),
        compiler_params=pltpu.CompilerParams(vmem_limit_bytes=44 * 2**20),
        name="top",
    )(arrived, samp, dense, w1, b1, w2, b2, w3, b3, wt, bh, wl, bl, labels)


def per_device(
    resident_row_blocks,
    orphan_blocks,
    home_offsets,
    home_lengths,
    home_samples,
    orphan_offsets,
    orphan_lengths,
    orphan_samples,
    orphan_owner,
    dense_inputs,
    labels,
    bottom_first,
    bias_first,
    bottom_second,
    bias_second,
    bottom_third,
    bias_third,
    top_hidden,
    bias_hidden,
    top_logit,
    bias_logit,
):
    chips = lax.axis_size("chip")
    devices = lax.axis_size("hst") * chips
    everyone = ("hst", "chip")
    homes, orphs = resident_row_blocks.shape[0], orphan_blocks.shape[0]
    height, width = resident_row_blocks.shape[1:]
    slots = (2 * orphs + chips - 1) // chips
    count = homes + orphs
    stride = -(-(count + 2) // 8) * 8

    me = lax.axis_index("chip")[None].astype(I32)
    parts = list(place(me, orphan_owner[:, 0], orphan_blocks, chips, slots))

    def send(shifts):
        for k in shifts:
            parts[k] = lax.ppermute(parts[k], "chip", [(c, (c + k) % chips) for c in range(chips)])

    order = sorted(range(1, chips), key=lambda k: abs(2 * k - chips))
    load, early = 0, []
    while 2.2 * (load + min(order[0], chips - order[0])) <= chips * chips // 4:
        k = order.pop(0)
        load += min(k, chips - k)
        early.append(k)
    send(early)

    offsets = jnp.concatenate([home_offsets, orphan_offsets], axis=0)
    lengths = jnp.concatenate([home_lengths, orphan_lengths], axis=0)
    samples = jnp.concatenate([home_samples, orphan_samples], axis=0)
    live = jnp.arange(offsets.shape[2], dtype=I32) < lengths[:, :, None]
    off = jnp.where(live, offsets, height).transpose(2, 0, 1).reshape(offsets.shape[2], -1)
    samp = jnp.pad(samples.T, ((0, 0), (0, 128 - count)))

    packed = pool(off, samp, resident_row_blocks, orphan_blocks, devices, stride)
    packed = packed.reshape(devices, stride, width)
    arrived = lax.all_to_all(packed, everyone, split_axis=0, concat_axis=0, tiled=True)

    held = lax.optimization_barrier((arrived, [parts[k] for k in order]))
    arrived = held[0]
    for k, part in zip(order, held[1]):
        parts[k] = part
    send(order)

    total = devices * count
    depth = -(-total // (F * 128)) * 128
    where = (arrived[:, count, :count].astype(F32) * 256.0
             + arrived[:, count + 1, :count].astype(F32)).astype(I32)
    where = jnp.concatenate([where[:, :homes].reshape(-1), where[:, homes:].reshape(-1)])
    where = jnp.pad(where, (0, F * depth - total), constant_values=-1).reshape(depth, F).T

    logits, loss = top(
        homes, orphs, depth, arrived, where, dense_inputs,
        bottom_first, bias_first[None], bottom_second, bias_second[None],
        bottom_third, bias_third[None], top_hidden, bias_hidden[None],
        top_logit.T.astype(F32), bias_logit, labels[None],
    )
    rehomed = gather(me, parts)
    losses = lax.all_to_all(loss[:, None, :], everyone, split_axis=0, concat_axis=0, tiled=True)
    return rehomed, logits[0], jnp.sum(losses[:, 0, 0])


def solution(mesh):
    both = ("hst", "chip")
    three, two = P(both, None, None), P(both, None)

    return jax.shard_map(
        per_device,
        mesh=mesh,
        in_specs=(three, three, three, two, two, three, two, two, two, two, P(both)) + (P(),) * 10,
        out_specs=(three, P(both), P()),
        check_vma=False,
    )
```
